32 devices in a mesh: mat: 4 (over y, z), row: 8 (over x, core).
Axes of the slice: x: 4, y: 2, z: 2, core: 2. Of those that a mesh axis runs over, the one named last changes fastest.
The devices are a block of a 4x4x8 slice.
Arguments:
- operand: bfloat16 [8192, 16384], P(('mat', 'row')), parts along dimension 0
Outputs:
- output 1: float32 [32, 5, 256, 256], P(('mat', 'row')), parts along dimension 0
- output 2: float32 [8192, 16384], P(('mat', 'row')), parts along dimension 0
There are 4 independent parts. The reference program is written for one: setup_inputs(seed, part) draws one part's arguments, and reference() takes and returns one part's arrays. A program takes and returns all parts, laid end to end along the dimension named above; each array names one.
All inputs are finite; a program needn't handle non-finite values.
Results may differ from the reference program's by a relative error of at most 0.001.
Values are sent between devices in bfloat16 or wider.
A program may use at most 768 MiB of HBM per device.

```python
import math
import jax
import jax.numpy as jnp

GRAM_ROWS = 2048
GRAM_COLS = 16384
GROUPS = 8
BLOCK_ROWS = GRAM_ROWS // GROUPS


def split_counts(groups):
    half_count = groups // 2
    low_count = 2 ** (int(math.log2(half_count)) // 2)
    return half_count, low_count, half_count // low_count


def slot_table(groups):
    half_count, low_count = split_counts(groups)[:2]
    rows_tab = []
    cols_tab = []
    for device in range(groups):
        row_list = [device]
        col_list = [device]
        for distance in range(1, half_count + 1):
            shift_off = ((distance + low_count - 1) // low_count) * low_count - distance
            first_blk = (device + shift_off) % groups
            second_blk = (first_blk + distance) % groups
            if distance == half_count and first_blk >= half_count:
                row_list.append(-1)
                col_list.append(-1)
            else:
                row_list.append(max(first_blk, second_blk))
                col_list.append(min(first_blk, second_blk))
        rows_tab.append(row_list)
        cols_tab.append(col_list)
    return rows_tab, cols_tab


def setup_inputs(seed: int = 0, part: int = 0) -> dict:
    part_key = jax.random.fold_in(jax.random.key(seed), part)
    key_vals, key_scale = jax.random.split(part_key)
    base_scale = (GRAM_COLS * (GRAM_ROWS + GRAM_COLS)) ** (-1.0 / 6.0)
    values = jax.random.normal(key_vals, (GROUPS, BLOCK_ROWS, GRAM_COLS), jnp.float32)
    block_scale = jax.random.uniform(key_scale, (GROUPS, 1, 1), jnp.float32, 0.5, 1.0)
    operand = (values * block_scale * base_scale).reshape(GRAM_ROWS, GRAM_COLS).astype(jnp.bfloat16)
    return {"operand": operand}


def reference(operand):
    full_gram = jnp.dot(operand, operand.T, preferred_element_type=jnp.float32)
    rows_tab, cols_tab = slot_table(GROUPS)
    row_index = jnp.array(rows_tab, jnp.int32)
    col_index = jnp.array(cols_tab, jnp.int32)
    is_valid = (row_index >= 0)[:, :, None, None]
    tile_grid = full_gram.reshape(GROUPS, BLOCK_ROWS, GROUPS, BLOCK_ROWS).transpose(0, 2, 1, 3)
    picked = tile_grid[jnp.maximum(row_index, 0), jnp.maximum(col_index, 0)]
    gram_blocks = jnp.where(is_valid, picked, 0.0)
    applied = jnp.dot(full_gram.astype(jnp.bfloat16), operand, preferred_element_type=jnp.float32)
    return gram_blocks, applied
```

```python
import functools

import jax
import jax.numpy as jnp
from jax import lax
from jax.experimental import pallas as pl
from jax.experimental.pallas import tpu as pltpu
from jax.sharding import PartitionSpec as P

BATCHES = 4
GRAM_STEP = 2048
APPLY_STEP = 1024
OUT_PARTS = 8
VMEM_LIMIT = 67043328

NT = (((1,), (1,)), ((), ()))


def kernel(groups, a_ref, y_ref, g_ref, hb, own, work, far, acc, y_acc, x_gram,
           own_send, own_recv, fwd_send, fwd_recv, relay_send, relay_recv,
           far_send, far_recv, load_sem, out_sem):
    rows, cols = a_ref.shape
    half = rows // 2
    piece = half // BATCHES
    me = lax.axis_index("row")
    core = lax.rem(me, 2)
    right = lax.rem(me + 2, groups)
    left = lax.rem(me + groups - 2, groups)
    sib = me + 1 - 2 * core

    def remote(src, dst, send, recv, to):
        return pltpu.make_async_remote_copy(
            src_ref=src, dst_ref=dst, send_sem=send, recv_sem=recv,
            device_id={"row": to}, device_id_type=pl.DeviceIdType.MESH)

    barrier = pltpu.get_barrier_semaphore()
    for peer in (left, right, sib):
        pl.semaphore_signal(barrier, inc=1, device_id={"row": peer}, device_id_type=pl.DeviceIdType.MESH)
    pl.semaphore_wait(barrier, 3)

    def half_rows(index):
        return pl.ds(index * half, half)

    to_right = [remote(a_ref.at[half_rows(s)], hb.at[1, half_rows(s)], own_send.at[s], own_recv.at[s], right) for s in (0, 1)]
    to_left = [remote(a_ref.at[half_rows(s)], hb.at[2, half_rows(s)], own_send.at[2 + s], own_recv.at[2 + s], left) for s in (0, 1)]
    to_sib = remote(a_ref, hb.at[0], own_send.at[4], own_recv.at[4], sib)
    to_right[0].start()
    to_left[1].start()
    to_right[1].start()
    to_left[0].start()
    to_sib.start()

    fwd_right = [remote(hb.at[1, pl.ds(i * piece, piece)], far.at[i, pl.ds(0, piece)],
                        fwd_send.at[i], fwd_recv.at[i], right) for i in range(BATCHES)]
    fwd_left = [remote(hb.at[2, pl.ds(half + i * piece, piece)], far.at[i, pl.ds(piece, piece)],
                       fwd_send.at[BATCHES + i], fwd_recv.at[BATCHES + i], left) for i in range(BATCHES)]
    relay = [[remote(hb.at[1 + side, half_rows(s)], hb.at[3 + side, half_rows(s)],
                     relay_send.at[2 * side + s], relay_recv.at[2 * side + s], sib) for s in (0, 1)] for side in (0, 1)]
    far_relay = [remote(far.at[i, pl.ds(0, 2 * piece)], far.at[i, pl.ds(2 * piece, 2 * piece)],
                        far_send.at[i], far_recv.at[i], sib) for i in range(BATCHES)]

    def gram_t(left_ref, right_ref, count, base=0):
        acc[pl.ds(base, count), :] = jnp.zeros((count, rows), jnp.float32)

        def body(step, carry):
            sl = pl.ds(pl.multiple_of(step * GRAM_STEP, GRAM_STEP), GRAM_STEP)
            acc[pl.ds(base, count), :] += lax.dot_general(
                left_ref[:, sl], right_ref[:, sl], NT, preferred_element_type=jnp.float32)
            return carry

        lax.fori_loop(0, cols // GRAM_STEP, body, 0)

    def apply(b_ref, count, first=False):
        coef = acc[pl.ds(0, count), :].astype(jnp.bfloat16).T

        def body(step, carry):
            sl = pl.ds(pl.multiple_of(step * APPLY_STEP, APPLY_STEP), APPLY_STEP)
            term = jnp.dot(coef, b_ref[:, sl], preferred_element_type=jnp.float32)
            y_acc[:, sl] = term if first else y_acc[:, sl] + term
            return carry

        lax.fori_loop(0, cols // APPLY_STEP, body, 0)

    def oriented(value, slot):
        distance = slot
        shift = slot % 2
        first_blk = lax.rem(me + shift, groups)
        return jnp.where(first_blk + distance >= groups, value.T, value)

    def load(src, dst, sem):
        copy = pltpu.make_async_copy(src, dst, sem)
        copy.start()
        return copy

    first_load = load(a_ref, own, load_sem.at[0])
    first_load.wait()
    gram_t(own, own, rows)
    g_ref[0] = acc[pl.ds(0, rows), :]
    apply(own, rows, first=True)

    to_sib.wait_recv()
    load(hb.at[0], work.at[pl.ds(0, rows)], load_sem.at[1]).wait()
    gram_t(work.at[pl.ds(0, rows)], own, rows)
    apply(work.at[pl.ds(0, rows)], rows)

    to_right[0].wait_recv()
    for copy in fwd_right:
        copy.start()
    relay[0][0].start()
    to_left[1].wait_recv()
    for copy in fwd_left:
        copy.start()
    relay[1][1].start()
    to_right[1].wait_recv()
    relay[0][1].start()
    to_left[0].wait_recv()
    relay[1][0].start()

    for side in (0, 1):
        one = load(hb.at[1 + side], work.at[pl.ds(0, rows)], load_sem.at[2 + 2 * side])
        relay[side][0].wait_recv()
        relay[side][1].wait_recv()
        two = load(hb.at[3 + side], work.at[pl.ds(rows, rows)], load_sem.at[3 + 2 * side])
        one.wait()
        two.wait()
        gram_t(work, own, 2 * rows)
        if side == 1:
            g_ref[2] = oriented(acc[pl.ds(0, rows), :], 2)
        apply(work, 2 * rows)

    load(hb.at[4 * core], work.at[pl.ds(rows, rows)], load_sem.at[6]).wait()
    x_block = work.at[pl.ds(rows, rows)]
    gram_t(work.at[pl.ds(0, rows)], x_block, rows)
    g_ref[1] = oriented(acc[pl.ds(0, rows), :], 1)

    stores = []
    for i in range(BATCHES):
        fwd_right[i].wait_recv()
        fwd_left[i].wait_recv()
        far_relay[i].start()
        gram_t(far.at[i, pl.ds(0, 2 * piece)], x_block, 2 * piece)
        for s in (0, 1):
            x_gram[pl.ds(s * half + i * piece, piece), :] = acc[pl.ds(s * piece, piece), :]
        far_relay[i].wait_recv()
        gram_t(far.at[i], own, 4 * piece)
        for s in (0, 1):
            part = acc[pl.ds(s * piece, piece), :]
            g_ref[4, pl.ds(s * half + i * piece, piece), :] = jnp.where(me >= groups // 2, 0.0, part)
        if i < BATCHES - 1:
            apply(far.at[i], 4 * piece)
        else:
            coef = acc[pl.ds(0, 4 * piece), :].astype(jnp.bfloat16).T
            width = cols // OUT_PARTS
            for part in range(OUT_PARTS):
                for sub in range(width // APPLY_STEP):
                    sl = pl.ds(part * width + sub * APPLY_STEP, APPLY_STEP)
                    y_acc[:, sl] += jnp.dot(coef, far[i, :, sl], preferred_element_type=jnp.float32)
                sl = pl.ds(part * width, width)
                copy = pltpu.make_async_copy(y_acc.at[:, sl], y_ref.at[:, sl], out_sem.at[part])
                copy.start()
                stores.append(copy)
    g_ref[3] = oriented(x_gram[...], 3)
    for copy in stores:
        copy.wait()
    for copy in to_right + to_left + [to_sib] + fwd_right + fwd_left + relay[0] + relay[1] + far_relay:
        copy.wait_send()


def solution(mesh):
    groups = mesh.shape["row"]

    def per_device(own_block):
        rows, cols = own_block.shape
        slots = groups // 2 + 1
        far_rows = 2 * rows // BATCHES
        dma = pltpu.SemaphoreType.DMA
        y, gram, _ = pl.pallas_call(
            functools.partial(kernel, groups),
            out_shape=(
                jax.ShapeDtypeStruct((rows, cols), jnp.float32),
                jax.ShapeDtypeStruct((slots, rows, rows), jnp.float32),
                jax.ShapeDtypeStruct((5, rows, cols), jnp.bfloat16),
            ),
            in_specs=[pl.BlockSpec(memory_space=pl.ANY)],
            out_specs=(
                pl.BlockSpec(memory_space=pl.ANY),
                pl.BlockSpec(memory_space=pltpu.VMEM),
                pl.BlockSpec(memory_space=pl.ANY),
            ),
            scratch_shapes=[
                pltpu.VMEM((rows, cols), jnp.bfloat16),
                pltpu.VMEM((2 * rows, cols), jnp.bfloat16),
                pltpu.VMEM((BATCHES, far_rows, cols), jnp.bfloat16),
                pltpu.VMEM((2 * rows, rows), jnp.float32),
                pltpu.VMEM((rows, cols), jnp.float32),
                pltpu.VMEM((rows, rows), jnp.float32),
                dma((5,)), dma((5,)),
                dma((2 * BATCHES,)), dma((2 * BATCHES,)),
                dma((4,)), dma((4,)),
                dma((BATCHES,)), dma((BATCHES,)),
                dma((7,)), dma((OUT_PARTS,)),
            ],
            compiler_params=pltpu.CompilerParams(
                collective_id=0, has_side_effects=True, vmem_limit_bytes=VMEM_LIMIT),
        )(own_block)
        return gram[None], y

    return jax.shard_map(
        per_device, mesh=mesh, in_specs=(P(("mat", "row"), None),),
        out_specs=(P(("mat", "row"), None, None, None), P(("mat", "row"), None)), check_vma=False)
```

```python
import functools

import jax
import jax.numpy as jnp
from jax import lax
from jax.experimental import pallas as pl
from jax.experimental.pallas import tpu as pltpu
from jax.sharding import PartitionSpec as P

BATCHES = 4
GRAM_STEP = 2048
APPLY_STEP = 1024
VMEM_LIMIT = 46 << 20

NT = (((1,), (1,)), ((), ()))


def kernel(groups, a_ref, y_acc, g_ref, hb, own, work, far, acc, x_gram,
           own_send, own_recv, fwd_send, fwd_recv, relay_send, relay_recv,
           far_send, far_recv, load_sem):
    rows, cols = a_ref.shape
    half = rows // 2
    piece = half // BATCHES
    me = lax.axis_index("row")
    core = lax.rem(me, 2)
    right = lax.rem(me + 2, groups)
    left = lax.rem(me + groups - 2, groups)
    sib = me + 1 - 2 * core

    def remote(src, dst, send, recv, to):
        return pltpu.make_async_remote_copy(
            src_ref=src, dst_ref=dst, send_sem=send, recv_sem=recv,
            device_id={"row": to}, device_id_type=pl.DeviceIdType.MESH)

    barrier = pltpu.get_barrier_semaphore()
    for peer in (left, right, sib):
        pl.semaphore_signal(barrier, inc=1, device_id={"row": peer}, device_id_type=pl.DeviceIdType.MESH)
    pl.semaphore_wait(barrier, 3)

    def half_rows(index):
        return pl.ds(index * half, half)

    to_right = [remote(a_ref.at[half_rows(s)], hb.at[1, half_rows(s)], own_send.at[s], own_recv.at[s], right) for s in (0, 1)]
    to_left = [remote(a_ref.at[half_rows(s)], hb.at[2, half_rows(s)], own_send.at[2 + s], own_recv.at[2 + s], left) for s in (0, 1)]
    to_sib = remote(a_ref, hb.at[0], own_send.at[4], own_recv.at[4], sib)
    to_right[0].start()
    to_left[1].start()
    to_right[1].start()
    to_left[0].start()
    to_sib.start()

    fwd_right = [remote(hb.at[1, pl.ds(i * piece, piece)], far.at[i, pl.ds(0, piece)],
                        fwd_send.at[i], fwd_recv.at[i], right) for i in range(BATCHES)]
    fwd_left = [remote(hb.at[2, pl.ds(half + i * piece, piece)], far.at[i, pl.ds(piece, piece)],
                       fwd_send.at[BATCHES + i], fwd_recv.at[BATCHES + i], left) for i in range(BATCHES)]
    relay = [[remote(hb.at[1 + side, half_rows(s)], hb.at[3 + side, half_rows(s)],
                     relay_send.at[2 * side + s], relay_recv.at[2 * side + s], sib) for s in (0, 1)] for side in (0, 1)]
    far_relay = [remote(far.at[i, pl.ds(0, 2 * piece)], far.at[i, pl.ds(2 * piece, 2 * piece)],
                        far_send.at[i], far_recv.at[i], sib) for i in range(BATCHES)]

    def gram_t(left_ref, right_ref, count, base=0):
        acc[pl.ds(base, count), :] = jnp.zeros((count, rows), jnp.float32)

        def body(step, carry):
            sl = pl.ds(pl.multiple_of(step * GRAM_STEP, GRAM_STEP), GRAM_STEP)
            acc[pl.ds(base, count), :] += lax.dot_general(
                left_ref[:, sl], right_ref[:, sl], NT, preferred_element_type=jnp.float32)
            return carry

        lax.fori_loop(0, cols // GRAM_STEP, body, 0)

    def apply(b_ref, count, first=False):
        coef = acc[pl.ds(0, count), :].astype(jnp.bfloat16).T

        def body(step, carry):
            sl = pl.ds(pl.multiple_of(step * APPLY_STEP, APPLY_STEP), APPLY_STEP)
            term = jnp.dot(coef, b_ref[:, sl], preferred_element_type=jnp.float32)
            y_acc[:, sl] = term if first else y_acc[:, sl] + term
            return carry

        lax.fori_loop(0, cols // APPLY_STEP, body, 0)

    def oriented(value, slot):
        distance = slot
        shift = slot % 2
        first_blk = lax.rem(me + shift, groups)
        return jnp.where(first_blk + distance >= groups, value.T, value)

    def load(src, dst, sem):
        copy = pltpu.make_async_copy(src, dst, sem)
        copy.start()
        return copy

    first_load = load(a_ref, own, load_sem.at[0])
    first_load.wait()
    gram_t(own, own, rows)
    g_ref[0] = acc[pl.ds(0, rows), :]
    apply(own, rows, first=True)

    to_sib.wait_recv()
    load(hb.at[0], work.at[pl.ds(0, rows)], load_sem.at[1]).wait()
    gram_t(work.at[pl.ds(0, rows)], own, rows)
    apply(work.at[pl.ds(0, rows)], rows)

    to_right[0].wait_recv()
    for copy in fwd_right:
        copy.start()
    relay[0][0].start()
    to_left[1].wait_recv()
    for copy in fwd_left:
        copy.start()
    relay[1][1].start()
    to_right[1].wait_recv()
    relay[0][1].start()
    to_left[0].wait_recv()
    relay[1][0].start()

    for side in (0, 1):
        one = load(hb.at[1 + side], work.at[pl.ds(0, rows)], load_sem.at[2 + 2 * side])
        relay[side][0].wait_recv()
        relay[side][1].wait_recv()
        two = load(hb.at[3 + side], work.at[pl.ds(rows, rows)], load_sem.at[3 + 2 * side])
        one.wait()
        two.wait()
        gram_t(work, own, 2 * rows)
        if side == 1:
            g_ref[2] = oriented(acc[pl.ds(0, rows), :], 2)
        apply(work, 2 * rows)

    load(hb.at[4 * core], work.at[pl.ds(rows, rows)], load_sem.at[6]).wait()
    x_block = work.at[pl.ds(rows, rows)]
    gram_t(work.at[pl.ds(0, rows)], x_block, rows)
    g_ref[1] = oriented(acc[pl.ds(0, rows), :], 1)

    for i in range(BATCHES):
        fwd_right[i].wait_recv()
        fwd_left[i].wait_recv()
        far_relay[i].start()
        gram_t(far.at[i, pl.ds(0, 2 * piece)], x_block, 2 * piece)
        for s in (0, 1):
            x_gram[pl.ds(s * half + i * piece, piece), :] = acc[pl.ds(s * piece, piece), :]
        far_relay[i].wait_recv()
        gram_t(far.at[i], own, 4 * piece)
        for s in (0, 1):
            part = acc[pl.ds(s * piece, piece), :]
            g_ref[4, pl.ds(s * half + i * piece, piece), :] = jnp.where(me >= groups // 2, 0.0, part)
        apply(far.at[i], 4 * piece)
    g_ref[3] = oriented(x_gram[...], 3)
    for copy in to_right + to_left + [to_sib] + fwd_right + fwd_left + relay[0] + relay[1] + far_relay:
        copy.wait_send()


def solution(mesh):
    groups = mesh.shape["row"]

    def per_device(own_block):
        rows, cols = own_block.shape
        slots = groups // 2 + 1
        far_rows = 2 * rows // BATCHES
        dma = pltpu.SemaphoreType.DMA
        y, gram, _ = pl.pallas_call(
            functools.partial(kernel, groups),
            out_shape=(
                pltpu.VMEM((rows, cols), jnp.float32),
                pltpu.VMEM((slots, rows, rows), jnp.float32),
                jax.ShapeDtypeStruct((5, rows, cols), jnp.bfloat16),
            ),
            in_specs=[pl.BlockSpec(memory_space=pl.ANY)],
            out_specs=(
                pl.BlockSpec(memory_space=pltpu.VMEM),
                pl.BlockSpec(memory_space=pltpu.VMEM),
                pl.BlockSpec(memory_space=pl.ANY),
            ),
            scratch_shapes=[
                pltpu.VMEM((rows, cols), jnp.bfloat16),
                pltpu.VMEM((2 * rows, cols), jnp.bfloat16),
                pltpu.VMEM((BATCHES, far_rows, cols), jnp.bfloat16),
                pltpu.VMEM((2 * rows, rows), jnp.float32),
                pltpu.VMEM((rows, rows), jnp.float32),
                dma((5,)), dma((5,)),
                dma((2 * BATCHES,)), dma((2 * BATCHES,)),
                dma((4,)), dma((4,)),
                dma((BATCHES,)), dma((BATCHES,)),
                dma((7,)),
            ],
            compiler_params=pltpu.CompilerParams(
                collective_id=0, has_side_effects=True, vmem_limit_bytes=VMEM_LIMIT),
        )(own_block)
        return gram[None], y

    return jax.shard_map(
        per_device, mesh=mesh, in_specs=(P(("mat", "row"), None),),
        out_specs=(P(("mat", "row"), None, None, None), P(("mat", "row"), None)), check_vma=False)
```

```python
import functools

import jax
import jax.numpy as jnp
from jax import lax
from jax.experimental import pallas as pl
from jax.experimental.pallas import tpu as pltpu
from jax.sharding import PartitionSpec as P

GRAM_STEP = 4096
APPLY_STEP = 2048
LAST_CHUNKS = 8
OUT_PARTS = 16
GATHER_VMEM = 40 << 20
FINISH_VMEM = 18 << 20

NT = (((1,), (1,)), ((), ()))


def piece_rows(half):
    return (half // 2, half // 4), half // 4


def oriented(me, groups, value, slot):
    first_blk = lax.rem(me + slot % 2, groups)
    return jnp.where(first_blk + slot >= groups, value.T, value)


def gather_kernel(groups, a_ref, y_ref, g_ref, tail_gram, tail, hb, own, work, far, acc,
                  own_send, own_recv, fwd_send, fwd_recv, relay_send, relay_recv,
                  far_send, far_recv, last_send, last_recv, tail_send, tail_recv, load_sem):
    rows, cols = a_ref.shape
    half = rows // 2
    early, late = piece_rows(half)
    me = lax.axis_index("row")
    core = lax.rem(me, 2)
    right = lax.rem(me + 2, groups)
    left = lax.rem(me + groups - 2, groups)
    sib = me + 1 - 2 * core

    def remote(src, dst, send, recv, to):
        return pltpu.make_async_remote_copy(
            src_ref=src, dst_ref=dst, send_sem=send, recv_sem=recv,
            device_id={"row": to}, device_id_type=pl.DeviceIdType.MESH)

    barrier = pltpu.get_barrier_semaphore()
    for peer in (left, right, sib):
        pl.semaphore_signal(barrier, inc=1, device_id={"row": peer}, device_id_type=pl.DeviceIdType.MESH)
    pl.semaphore_wait(barrier, 3)

    def half_rows(index):
        return pl.ds(index * half, half)

    to_right = [remote(a_ref.at[half_rows(s)], hb.at[1, half_rows(s)], own_send.at[s], own_recv.at[s], right) for s in (0, 1)]
    to_left = [remote(a_ref.at[half_rows(s)], hb.at[2, half_rows(s)], own_send.at[2 + s], own_recv.at[2 + s], left) for s in (0, 1)]
    to_sib = remote(a_ref, hb.at[0], own_send.at[4], own_recv.at[4], sib)
    to_right[0].start()
    to_left[1].start()
    to_right[1].start()
    to_left[0].start()
    to_sib.start()

    fwd, far_relay, batch, offset = [], [], [], 0
    for i, piece in enumerate(early):
        base = 4 * offset
        batch.append(far.at[pl.ds(base, 4 * piece)])
        fwd.append([remote(hb.at[1 + side, pl.ds(side * half + offset, piece)], far.at[pl.ds(base + side * piece, piece)],
                           fwd_send.at[2 * i + side], fwd_recv.at[2 * i + side], (right, left)[side]) for side in (0, 1)])
        far_relay.append(remote(far.at[pl.ds(base, 2 * piece)], far.at[pl.ds(base + 2 * piece, 2 * piece)],
                                far_send.at[i], far_recv.at[i], sib))
        offset += piece
    late_offset = offset
    width = cols // LAST_CHUNKS
    last, tail_relay = [], []
    for q in range(LAST_CHUNKS):
        sl = pl.ds(q * width, width)
        last.append([remote(hb.at[1 + side, pl.ds(side * half + late_offset, late), sl], tail.at[pl.ds(side * late, late), sl],
                            last_send.at[2 * q + side], last_recv.at[2 * q + side], (right, left)[side]) for side in (0, 1)])
        tail_relay.append(remote(tail.at[pl.ds(0, 2 * late), sl], tail.at[pl.ds(2 * late, 2 * late), sl],
                                 tail_send.at[q], tail_recv.at[q], sib))
    relay = [[remote(hb.at[1 + side, half_rows(s)], hb.at[3 + side, half_rows(s)],
                     relay_send.at[2 * side + s], relay_recv.at[2 * side + s], sib) for s in (0, 1)] for side in (0, 1)]

    def gram_t(left_ref, right_ref, count):
        acc[pl.ds(0, count), :] = jnp.zeros((count, rows), jnp.float32)

        def body(step, carry):
            sl = pl.ds(pl.multiple_of(step * GRAM_STEP, GRAM_STEP), GRAM_STEP)
            acc[pl.ds(0, count), :] += lax.dot_general(
                left_ref[:, sl], right_ref[:, sl], NT, preferred_element_type=jnp.float32)
            return carry

        lax.fori_loop(0, cols // GRAM_STEP, body, 0)

    def apply(b_ref, count, first=False):
        coef = acc[pl.ds(0, count), :].astype(jnp.bfloat16).T

        def body(step, carry):
            sl = pl.ds(pl.multiple_of(step * APPLY_STEP, APPLY_STEP), APPLY_STEP)
            term = jnp.dot(coef, b_ref[:, sl], preferred_element_type=jnp.float32)
            y_ref[:, sl] = term if first else y_ref[:, sl] + term
            return carry

        lax.fori_loop(0, cols // APPLY_STEP, body, 0)

    def load(src, dst, sem):
        copy = pltpu.make_async_copy(src, dst, sem)
        copy.start()
        return copy

    lower, upper = work.at[pl.ds(0, rows)], work.at[pl.ds(rows, rows)]
    load(a_ref, own, load_sem.at[0]).wait()
    gram_t(own, own, rows)
    g_ref[0] = acc[pl.ds(0, rows), :]
    apply(own, rows, first=True)

    to_sib.wait_recv()
    load(hb.at[0], lower, load_sem.at[1]).wait()
    gram_t(lower, own, rows)
    apply(lower, rows)

    for turn in (0, 1):
        arrivals = (to_right[turn], to_left[1 - turn])
        for copy in arrivals:
            copy.wait_recv()
        if turn == 0:
            for pair in fwd + last:
                for copy in pair:
                    copy.start()
        picks = (relay[0][turn], relay[1][1 - turn])
        for copy in picks:
            copy.start()
        halves = (half_rows(turn), half_rows(1 - turn))
        loads = [load(hb.at[1 + side, halves[side]], work.at[half_rows(side)], load_sem.at[2 + 4 * turn + side]) for side in (0, 1)]
        for side, copy in enumerate(picks):
            copy.wait_recv()
            loads.append(load(hb.at[3 + side, halves[side]], work.at[half_rows(2 + side)], load_sem.at[4 + 4 * turn + side]))
        for copy in loads:
            copy.wait()
        gram_t(work, own, 2 * rows)
        g_ref[2, halves[1], :] = acc[half_rows(1), :]
        apply(work, 2 * rows)
    g_ref[2] = oriented(me, groups, g_ref[2], 2)

    pair_loads = [load(hb.at[2], lower, load_sem.at[10]), load(hb.at[4 * core], upper, load_sem.at[11])]

    def keep_slot(value, row, count):
        g_ref[4, pl.ds(row, count), :] = jnp.where(me >= groups // 2, 0.0, value)

    def next_gram(piece, offset):
        gram_t(far.at[pl.ds(4 * offset, 2 * piece)], upper, 2 * piece)
        for s in (0, 1):
            g_ref[3, pl.ds(s * half + offset, piece), :] = acc[pl.ds(s * piece, piece), :]

    offset = 0
    for i, piece in enumerate(early):
        for copy in fwd[i]:
            copy.wait_recv()
        far_relay[i].start()
        if i > 0:
            next_gram(piece, offset)
        far_relay[i].wait_recv()
        gram_t(batch[i], own, 4 * piece)
        for s in (0, 1):
            keep_slot(acc[pl.ds(s * piece, piece), :], s * half + offset, piece)
        apply(batch[i], 4 * piece)
        if i == 0:
            for copy in pair_loads:
                copy.wait()
            gram_t(lower, upper, rows)
            g_ref[1] = oriented(me, groups, acc[pl.ds(0, rows), :], 1)
            next_gram(piece, offset)
        offset += piece

    near_rows, relay_rows = pl.ds(0, 2 * late), pl.ds(2 * late, 2 * late)

    def add(target, where, q, right_ref):
        sl = pl.ds(q * width, width)
        value = lax.dot_general(tail[where, sl], right_ref[:, sl], NT, preferred_element_type=jnp.float32)
        target[where, :] = value if q == 0 else target[where, :] + value

    for q in range(LAST_CHUNKS + 1):
        if q < LAST_CHUNKS:
            for copy in last[q]:
                copy.wait_recv()
            tail_relay[q].start()
            add(tail_gram, near_rows, q, own)
            add(acc, near_rows, q, upper)
        if q > 0:
            tail_relay[q - 1].wait_recv()
            add(tail_gram, relay_rows, q - 1, own)
    for s in (0, 1):
        g_ref[3, pl.ds(s * half + late_offset, late), :] = acc[pl.ds(s * late, late), :]
        keep_slot(tail_gram[pl.ds(s * late, late), :], s * half + late_offset, late)

    sent = to_right + to_left + [to_sib] + relay[0] + relay[1] + far_relay + tail_relay
    for copy in sent + [copy for pair in fwd + last for copy in pair]:
        copy.wait_send()


def finish_kernel(groups, y_ref, g_ref, tail_gram, tail, y_out, g_out, stage, turned, y_sem, g_sem):
    cols = y_ref.shape[1]
    coef = tail_gram[...].astype(jnp.bfloat16).T
    width = cols // OUT_PARTS
    copies = []
    for part in range(OUT_PARTS):
        sl = pl.ds(part * width, width)
        stage[:, sl] = y_ref[:, sl] + jnp.dot(coef, tail[:, sl], preferred_element_type=jnp.float32)
        copy = pltpu.make_async_copy(stage.at[:, sl], y_out.at[:, sl], y_sem.at[part])
        copy.start()
        copies.append(copy)
    turned[...] = oriented(lax.axis_index("row"), groups, g_ref[3], 3)
    for index, (src, slots) in enumerate(((g_ref.at[0:3], slice(0, 3)), (turned, 3), (g_ref.at[4], 4))):
        copy = pltpu.make_async_copy(src, g_out.at[slots], g_sem.at[index])
        copy.start()
        copies.append(copy)
    for copy in copies:
        copy.wait()


def solution(mesh):
    groups = mesh.shape["row"]

    def per_device(own_block):
        rows, cols = own_block.shape
        slots = groups // 2 + 1
        early, late = piece_rows(rows // 2)
        dma = pltpu.SemaphoreType.DMA
        whole = pl.BlockSpec(memory_space=pltpu.VMEM)
        raw = pl.BlockSpec(memory_space=pl.ANY)
        y_part, gram, tail_gram, tail, _ = pl.pallas_call(
            functools.partial(gather_kernel, groups),
            out_shape=(
                pltpu.VMEM((rows, cols), jnp.float32),
                pltpu.VMEM((slots, rows, rows), jnp.float32),
                pltpu.VMEM((4 * late, rows), jnp.float32),
                pltpu.VMEM((4 * late, cols), jnp.bfloat16),
                jax.ShapeDtypeStruct((5, rows, cols), jnp.bfloat16),
            ),
            in_specs=[raw],
            out_specs=(whole, whole, whole, whole, raw),
            scratch_shapes=[
                pltpu.VMEM((rows, cols), jnp.bfloat16),
                pltpu.VMEM((2 * rows, cols), jnp.bfloat16),
                pltpu.VMEM((4 * sum(early), cols), jnp.bfloat16),
                pltpu.VMEM((2 * rows, rows), jnp.float32),
                dma((5,)), dma((5,)),
                dma((2 * len(early),)), dma((2 * len(early),)),
                dma((4,)), dma((4,)),
                dma((len(early),)), dma((len(early),)),
                dma((2 * LAST_CHUNKS,)), dma((2 * LAST_CHUNKS,)),
                dma((LAST_CHUNKS,)), dma((LAST_CHUNKS,)),
                dma((12,)),
            ],
            compiler_params=pltpu.CompilerParams(
                collective_id=0, has_side_effects=True, vmem_limit_bytes=GATHER_VMEM),
        )(own_block)
        applied, gram = pl.pallas_call(
            functools.partial(finish_kernel, groups),
            out_shape=(
                jax.ShapeDtypeStruct((rows, cols), jnp.float32),
                jax.ShapeDtypeStruct((slots, rows, rows), jnp.float32),
            ),
            in_specs=[whole, whole, whole, whole],
            out_specs=(raw, raw),
            scratch_shapes=[pltpu.VMEM((rows, cols), jnp.float32), pltpu.VMEM((rows, rows), jnp.float32), dma((OUT_PARTS,)), dma((3,))],
            compiler_params=pltpu.CompilerParams(vmem_limit_bytes=FINISH_VMEM),
        )(y_part, gram, tail_gram, tail)
        return gram[None], applied

    return jax.shard_map(
        per_device, mesh=mesh, in_specs=(P(("mat", "row"), None),),
        out_specs=(P(("mat", "row"), None, None, None), P(("mat", "row"), None)), check_vma=False)
```

```python
import functools

import jax
import jax.numpy as jnp
from jax import lax
from jax.experimental import pallas as pl
from jax.experimental.pallas import tpu as pltpu
from jax.sharding import PartitionSpec as P

GRAM_STEP = 4096
APPLY_STEP = 2048
LAST_CHUNKS = 8
OUT_PARTS = 16
GATHER_VMEM = 40 << 20
FINISH_VMEM = 18 << 20

NT = (((1,), (1,)), ((), ()))


def piece_rows(half):
    return (half // 2, half // 4), half // 4


def oriented(me, groups, value, slot):
    first_blk = lax.rem(me + slot % 2, groups)
    return jnp.where(first_blk + slot >= groups, value.T, value)


def gather_kernel(groups, a_ref, y_ref, g_ref, tail_gram, tail, hb, own, work, far, acc,
                  own_send, own_recv, fwd_send, fwd_recv, relay_send, relay_recv,
                  far_send, far_recv, last_send, last_recv, tail_send, tail_recv, load_sem):
    rows, cols = a_ref.shape
    half = rows // 2
    early, late = piece_rows(half)
    me = lax.axis_index("row")
    core = lax.rem(me, 2)
    right = lax.rem(me + 2, groups)
    left = lax.rem(me + groups - 2, groups)
    sib = me + 1 - 2 * core

    def remote(src, dst, send, recv, to):
        return pltpu.make_async_remote_copy(
            src_ref=src, dst_ref=dst, send_sem=send, recv_sem=recv,
            device_id={"row": to}, device_id_type=pl.DeviceIdType.MESH)

    barrier = pltpu.get_barrier_semaphore()
    for peer in (left, right, sib):
        pl.semaphore_signal(barrier, inc=1, device_id={"row": peer}, device_id_type=pl.DeviceIdType.MESH)
    pl.semaphore_wait(barrier, 3)

    def half_rows(index):
        return pl.ds(index * half, half)

    to_right = [remote(a_ref.at[half_rows(s)], hb.at[1, half_rows(s)], own_send.at[s], own_recv.at[s], right) for s in (0, 1)]
    to_left = [remote(a_ref.at[half_rows(s)], hb.at[2, half_rows(s)], own_send.at[2 + s], own_recv.at[2 + s], left) for s in (0, 1)]
    to_sib = remote(a_ref, hb.at[0], own_send.at[4], own_recv.at[4], sib)
    to_right[0].start()
    to_left[1].start()
    to_right[1].start()
    to_left[0].start()
    to_sib.start()

    fwd, far_relay, batch, offset = [], [], [], 0
    for i, piece in enumerate(early):
        base = 4 * offset
        batch.append(far.at[pl.ds(base, 4 * piece)])
        fwd.append([remote(hb.at[1 + side, pl.ds(side * half + offset, piece)], far.at[pl.ds(base + side * piece, piece)],
                           fwd_send.at[2 * i + side], fwd_recv.at[2 * i + side], (right, left)[side]) for side in (0, 1)])
        far_relay.append(remote(far.at[pl.ds(base, 2 * piece)], far.at[pl.ds(base + 2 * piece, 2 * piece)],
                                far_send.at[i], far_recv.at[i], sib))
        offset += piece
    late_offset = offset
    width = cols // LAST_CHUNKS
    last, tail_relay = [], []
    for q in range(LAST_CHUNKS):
        sl = pl.ds(q * width, width)
        last.append([remote(hb.at[1 + side, pl.ds(side * half + late_offset, late), sl], tail.at[pl.ds(side * late, late), sl],
                            last_send.at[2 * q + side], last_recv.at[2 * q + side], (right, left)[side]) for side in (0, 1)])
        tail_relay.append(remote(tail.at[pl.ds(0, 2 * late), sl], tail.at[pl.ds(2 * late, 2 * late), sl],
                                 tail_send.at[q], tail_recv.at[q], sib))
    relay = [[remote(hb.at[1 + side, half_rows(s)], hb.at[3 + side, half_rows(s)],
                     relay_send.at[2 * side + s], relay_recv.at[2 * side + s], sib) for s in (0, 1)] for side in (0, 1)]

    def gram_t(left_ref, right_ref, count):
        acc[pl.ds(0, count), :] = jnp.zeros((count, rows), jnp.float32)

        def body(step, carry):
            sl = pl.ds(pl.multiple_of(step * GRAM_STEP, GRAM_STEP), GRAM_STEP)
            acc[pl.ds(0, count), :] += lax.dot_general(
                left_ref[:, sl], right_ref[:, sl], NT, preferred_element_type=jnp.float32)
            return carry

        lax.fori_loop(0, cols // GRAM_STEP, body, 0)

    def apply(b_ref, count, first=False):
        coef = acc[pl.ds(0, count), :].astype(jnp.bfloat16).T

        def body(step, carry):
            sl = pl.ds(pl.multiple_of(step * APPLY_STEP, APPLY_STEP), APPLY_STEP)
            term = jnp.dot(coef, b_ref[:, sl], preferred_element_type=jnp.float32)
            y_ref[:, sl] = term if first else y_ref[:, sl] + term
            return carry

        lax.fori_loop(0, cols // APPLY_STEP, body, 0)

    def load(src, dst, sem):
        copy = pltpu.make_async_copy(src, dst, sem)
        copy.start()
        return copy

    lower, upper = work.at[pl.ds(0, rows)], work.at[pl.ds(rows, rows)]
    load(a_ref, own, load_sem.at[0]).wait()
    gram_t(own, own, rows)
    g_ref[0] = acc[pl.ds(0, rows), :]
    apply(own, rows, first=True)

    to_sib.wait_recv()
    load(hb.at[0], lower, load_sem.at[1]).wait()
    gram_t(lower, own, rows)
    apply(lower, rows)

    for turn in (0, 1):
        arrivals = (to_right[turn], to_left[1 - turn])
        for copy in arrivals:
            copy.wait_recv()
        if turn == 0:
            for pair in fwd + last:
                for copy in pair:
                    copy.start()
        picks = (relay[0][turn], relay[1][1 - turn])
        for copy in picks:
            copy.start()
        halves = (half_rows(turn), half_rows(1 - turn))
        loads = [load(hb.at[1 + side, halves[side]], work.at[half_rows(side)], load_sem.at[2 + 4 * turn + side]) for side in (0, 1)]
        for side, copy in enumerate(picks):
            copy.wait_recv()
            loads.append(load(hb.at[3 + side, halves[side]], work.at[half_rows(2 + side)], load_sem.at[4 + 4 * turn + side]))
        for copy in loads:
            copy.wait()
        gram_t(work, own, 2 * rows)
        g_ref[2, halves[1], :] = acc[half_rows(1), :]
        apply(work, 2 * rows)
    g_ref[2] = oriented(me, groups, g_ref[2], 2)

    pair_loads = [load(hb.at[2], lower, load_sem.at[10]), load(hb.at[4 * core], upper, load_sem.at[11])]

    def keep_slot(value, row, count):
        g_ref[4, pl.ds(row, count), :] = jnp.where(me >= groups // 2, 0.0, value)

    def next_gram(piece, offset):
        gram_t(far.at[pl.ds(4 * offset, 2 * piece)], upper, 2 * piece)
        for s in (0, 1):
            g_ref[3, pl.ds(s * half + offset, piece), :] = acc[pl.ds(s * piece, piece), :]

    offset = 0
    for i, piece in enumerate(early):
        for copy in fwd[i]:
            copy.wait_recv()
        far_relay[i].start()
        if i > 0:
            next_gram(piece, offset)
        far_relay[i].wait_recv()
        gram_t(batch[i], own, 4 * piece)
        for s in (0, 1):
            keep_slot(acc[pl.ds(s * piece, piece), :], s * half + offset, piece)
        apply(batch[i], 4 * piece)
        if i == 0:
            for copy in pair_loads:
                copy.wait()
            gram_t(lower, upper, rows)
            g_ref[1] = oriented(me, groups, acc[pl.ds(0, rows), :], 1)
            next_gram(piece, offset)
        offset += piece

    near_rows, relay_rows = pl.ds(0, 2 * late), pl.ds(2 * late, 2 * late)

    def add(target, where, q, right_ref):
        sl = pl.ds(q * width, width)
        value = lax.dot_general(tail[where, sl], right_ref[:, sl], NT, preferred_element_type=jnp.float32)
        target[where, :] = value if q == 0 else target[where, :] + value

    for q in range(LAST_CHUNKS + 1):
        if q < LAST_CHUNKS:
            for copy in last[q]:
                copy.wait_recv()
            tail_relay[q].start()
            add(tail_gram, near_rows, q, own)
            add(acc, near_rows, q, upper)
        if q > 0:
            tail_relay[q - 1].wait_recv()
            add(tail_gram, relay_rows, q - 1, own)
    for s in (0, 1):
        g_ref[3, pl.ds(s * half + late_offset, late), :] = acc[pl.ds(s * late, late), :]
        keep_slot(tail_gram[pl.ds(s * late, late), :], s * half + late_offset, late)
    g_ref[3] = oriented(me, groups, g_ref[3], 3)

    sent = to_right + to_left + [to_sib] + relay[0] + relay[1] + far_relay + tail_relay
    for copy in sent + [copy for pair in fwd + last for copy in pair]:
        copy.wait_send()


def finish_kernel(y_ref, g_ref, tail_gram, tail, y_out, g_out, stage, y_sem, g_sem):
    cols = y_ref.shape[1]
    copies = [pltpu.make_async_copy(g_ref, g_out, g_sem)]
    copies[0].start()
    coef = tail_gram[...].astype(jnp.bfloat16).T
    width = cols // OUT_PARTS
    for part in range(OUT_PARTS):
        sl = pl.ds(part * width, width)
        stage[:, sl] = y_ref[:, sl] + jnp.dot(coef, tail[:, sl], preferred_element_type=jnp.float32)
        copy = pltpu.make_async_copy(stage.at[:, sl], y_out.at[:, sl], y_sem.at[part])
        copy.start()
        copies.append(copy)
    for copy in copies:
        copy.wait()


def solution(mesh):
    groups = mesh.shape["row"]

    def per_device(own_block):
        rows, cols = own_block.shape
        slots = groups // 2 + 1
        early, late = piece_rows(rows // 2)
        dma = pltpu.SemaphoreType.DMA
        whole = pl.BlockSpec(memory_space=pltpu.VMEM)
        raw = pl.BlockSpec(memory_space=pl.ANY)
        y_part, gram, tail_gram, tail, _ = pl.pallas_call(
            functools.partial(gather_kernel, groups),
            out_shape=(
                pltpu.VMEM((rows, cols), jnp.float32),
                pltpu.VMEM((slots, rows, rows), jnp.float32),
                pltpu.VMEM((4 * late, rows), jnp.float32),
                pltpu.VMEM((4 * late, cols), jnp.bfloat16),
                jax.ShapeDtypeStruct((5, rows, cols), jnp.bfloat16),
            ),
            in_specs=[raw],
            out_specs=(whole, whole, whole, whole, raw),
            scratch_shapes=[
                pltpu.VMEM((rows, cols), jnp.bfloat16),
                pltpu.VMEM((2 * rows, cols), jnp.bfloat16),
                pltpu.VMEM((4 * sum(early), cols), jnp.bfloat16),
                pltpu.VMEM((2 * rows, rows), jnp.float32),
                dma((5,)), dma((5,)),
                dma((2 * len(early),)), dma((2 * len(early),)),
                dma((4,)), dma((4,)),
                dma((len(early),)), dma((len(early),)),
                dma((2 * LAST_CHUNKS,)), dma((2 * LAST_CHUNKS,)),
                dma((LAST_CHUNKS,)), dma((LAST_CHUNKS,)),
                dma((12,)),
            ],
            compiler_params=pltpu.CompilerParams(
                collective_id=0, has_side_effects=True, vmem_limit_bytes=GATHER_VMEM),
        )(own_block)
        applied, gram = pl.pallas_call(
            finish_kernel,
            out_shape=(
                jax.ShapeDtypeStruct((rows, cols), jnp.float32),
                jax.ShapeDtypeStruct((slots, rows, rows), jnp.float32),
            ),
            in_specs=[whole, whole, whole, whole],
            out_specs=(raw, raw),
            scratch_shapes=[pltpu.VMEM((rows, cols), jnp.float32), dma((OUT_PARTS,)), dma],
            compiler_params=pltpu.CompilerParams(vmem_limit_bytes=FINISH_VMEM),
        )(y_part, gram, tail_gram, tail)
        return gram[None], applied

    return jax.shard_map(
        per_device, mesh=mesh, in_specs=(P(("mat", "row"), None),),
        out_specs=(P(("mat", "row"), None, None, None), P(("mat", "row"), None)), check_vma=False)
```

```python
import functools

import jax
import jax.numpy as jnp
from jax import lax
from jax.experimental import pallas as pl
from jax.experimental.pallas import tpu as pltpu
from jax.sharding import PartitionSpec as P

GRAM_STEP = 4096
APPLY_STEP = 2048
LAST_PARTS = (4, 4, 4, 4, 4, 4, 2, 4, 2)
LEADS = 2
OUT_PARTS = 16
GATHER_VMEM = 40 << 20
FINISH_VMEM = 18 << 20

NT = (((1,), (1,)), ((), ()))


def piece_rows(half):
    return (half // 2, half // 4), half // 4


def oriented(me, groups, value, slot):
    first_blk = lax.rem(me + slot % 2, groups)
    return jnp.where(first_blk + slot >= groups, value.T, value)


def gather_kernel(groups, a_ref, y_ref, g_ref, tail_gram, tail, hb, own, work, far, acc,
                  own_send, own_recv, fwd_send, fwd_recv, relay_send, relay_recv,
                  far_send, far_recv, last_send, last_recv, tail_send, tail_recv, lead_send, lead_recv, load_sem):
    rows, cols = a_ref.shape
    half = rows // 2
    early, late = piece_rows(half)
    me = lax.axis_index("row")
    core = lax.rem(me, 2)
    right = lax.rem(me + 2, groups)
    left = lax.rem(me + groups - 2, groups)
    sib = me + 1 - 2 * core

    def remote(src, dst, send, recv, to):
        return pltpu.make_async_remote_copy(
            src_ref=src, dst_ref=dst, send_sem=send, recv_sem=recv,
            device_id={"row": to}, device_id_type=pl.DeviceIdType.MESH)

    barrier = pltpu.get_barrier_semaphore()
    for peer in (left, right, sib):
        pl.semaphore_signal(barrier, inc=1, device_id={"row": peer}, device_id_type=pl.DeviceIdType.MESH)
    pl.semaphore_wait(barrier, 3)

    def half_rows(index):
        return pl.ds(index * half, half)

    to_right = [remote(a_ref.at[half_rows(s)], hb.at[1, half_rows(s)], own_send.at[s], own_recv.at[s], right) for s in (0, 1)]
    to_left = [remote(a_ref.at[half_rows(s)], hb.at[2, half_rows(s)], own_send.at[2 + s], own_recv.at[2 + s], left) for s in (0, 1)]
    to_sib = remote(a_ref, hb.at[0], own_send.at[4], own_recv.at[4], sib)
    to_right[0].start()
    to_left[1].start()
    to_right[1].start()
    to_left[0].start()
    to_sib.start()

    fwd, far_relay, batch, offset = [], [], [], 0
    for i, piece in enumerate(early):
        base = 4 * offset
        batch.append(far.at[pl.ds(base, 4 * piece)])
        fwd.append([remote(hb.at[1 + side, pl.ds(side * half + offset, piece)], far.at[pl.ds(base + side * piece, piece)],
                           fwd_send.at[2 * i + side], fwd_recv.at[2 * i + side], (right, left)[side]) for side in (0, 1)])
        far_relay.append(remote(far.at[pl.ds(base, 2 * piece)], far.at[pl.ds(base + 2 * piece, 2 * piece)],
                                far_send.at[i], far_recv.at[i], sib))
        offset += piece
    late_offset = offset
    count, unit = len(LAST_PARTS), cols // sum(LAST_PARTS)
    spans = [pl.ds(sum(LAST_PARTS[:q]) * unit, LAST_PARTS[q] * unit) for q in range(count)]
    last, tail_relay = [], []
    shared = count - LEADS
    for q, sl in enumerate(spans[:shared]):
        last.append([remote(hb.at[1 + side, pl.ds(side * half + late_offset, late), sl], tail.at[pl.ds(side * late, late), sl],
                            last_send.at[2 * q + side], last_recv.at[2 * q + side], (right, left)[side]) for side in (0, 1)])
        tail_relay.append(remote(tail.at[pl.ds(0, 2 * late), sl], tail.at[pl.ds(2 * late, 2 * late), sl],
                                 tail_send.at[q], tail_recv.at[q], sib))
    lead, lead_relay = [], []
    for q, sl in enumerate(spans[shared:]):
        lead.append([remote(hb.at[slot, pl.ds(side * half + late_offset, late), sl], tail.at[pl.ds((slot - 1) * late, late), sl],
                            lead_send.at[6 * q + slot - 1], lead_recv.at[6 * q + slot - 1], (right, left)[side])
                     for slot, side in ((1, 0), (2, 1), (3, 0), (4, 1))])
        lead_relay.append([remote(tail.at[pl.ds(2 * late * i, 2 * late), sl], tail.at[pl.ds(2 * late * (1 - i), 2 * late), sl],
                                  lead_send.at[6 * q + 4 + i], lead_recv.at[6 * q + 4 + i], sib) for i in (0, 1)])
    relay = [[remote(hb.at[1 + side, half_rows(s)], hb.at[3 + side, half_rows(s)],
                     relay_send.at[2 * side + s], relay_recv.at[2 * side + s], sib) for s in (0, 1)] for side in (0, 1)]

    def gram_t(left_ref, right_ref, count):
        acc[pl.ds(0, count), :] = jnp.zeros((count, rows), jnp.float32)

        def body(step, carry):
            sl = pl.ds(pl.multiple_of(step * GRAM_STEP, GRAM_STEP), GRAM_STEP)
            acc[pl.ds(0, count), :] += lax.dot_general(
                left_ref[:, sl], right_ref[:, sl], NT, preferred_element_type=jnp.float32)
            return carry

        lax.fori_loop(0, cols // GRAM_STEP, body, 0)

    def apply(b_ref, count, first=False):
        coef = acc[pl.ds(0, count), :].astype(jnp.bfloat16).T

        def body(step, carry):
            sl = pl.ds(pl.multiple_of(step * APPLY_STEP, APPLY_STEP), APPLY_STEP)
            term = jnp.dot(coef, b_ref[:, sl], preferred_element_type=jnp.float32)
            y_ref[:, sl] = term if first else y_ref[:, sl] + term
            return carry

        lax.fori_loop(0, cols // APPLY_STEP, body, 0)

    def load(src, dst, sem):
        copy = pltpu.make_async_copy(src, dst, sem)
        copy.start()
        return copy

    lower, upper = work.at[pl.ds(0, rows)], work.at[pl.ds(rows, rows)]
    load(a_ref, own, load_sem.at[0]).wait()
    gram_t(own, own, rows)
    g_ref[0] = acc[pl.ds(0, rows), :]
    apply(own, rows, first=True)

    to_sib.wait_recv()
    load(hb.at[0], lower, load_sem.at[1]).wait()
    gram_t(lower, own, rows)
    apply(lower, rows)

    for turn in (0, 1):
        arrivals = (to_right[turn], to_left[1 - turn])
        for copy in arrivals:
            copy.wait_recv()
        if turn == 0:
            for pair in fwd + last:
                for copy in pair:
                    copy.start()
        picks = (relay[0][turn], relay[1][1 - turn])
        for copy in picks:
            copy.start()
        halves = (half_rows(turn), half_rows(1 - turn))
        loads = [load(hb.at[1 + side, halves[side]], work.at[half_rows(side)], load_sem.at[2 + 4 * turn + side]) for side in (0, 1)]
        for side, copy in enumerate(picks):
            copy.wait_recv()
            loads.append(load(hb.at[3 + side, halves[side]], work.at[half_rows(2 + side)], load_sem.at[4 + 4 * turn + side]))
        if turn == 0:
            @pl.when(core == 1)
            def _():
                for copy in sum(lead, []):
                    copy.start()
        for copy in loads:
            copy.wait()
        gram_t(work, own, 2 * rows)
        g_ref[2, halves[1], :] = acc[half_rows(1), :]
        apply(work, 2 * rows)
    g_ref[2] = oriented(me, groups, g_ref[2], 2)

    pair_loads = [load(hb.at[2], lower, load_sem.at[10]), load(hb.at[4 * core], upper, load_sem.at[11])]

    def keep_slot(value, row, count):
        g_ref[4, pl.ds(row, count), :] = jnp.where(me >= groups // 2, 0.0, value)

    def next_gram(piece, offset):
        gram_t(far.at[pl.ds(4 * offset, 2 * piece)], upper, 2 * piece)
        for s in (0, 1):
            g_ref[3, pl.ds(s * half + offset, piece), :] = acc[pl.ds(s * piece, piece), :]

    offset = 0
    for i, piece in enumerate(early):
        for copy in fwd[i]:
            copy.wait_recv()
        far_relay[i].start()
        if i > 0:
            next_gram(piece, offset)
        far_relay[i].wait_recv()
        gram_t(batch[i], own, 4 * piece)
        for s in (0, 1):
            keep_slot(acc[pl.ds(s * piece, piece), :], s * half + offset, piece)
        apply(batch[i], 4 * piece)
        if i == 0:
            for copy in pair_loads:
                copy.wait()
            gram_t(lower, upper, rows)
            g_ref[1] = oriented(me, groups, acc[pl.ds(0, rows), :], 1)
            next_gram(piece, offset)
        offset += piece

    near_rows, relay_rows = pl.ds(0, 2 * late), pl.ds(2 * late, 2 * late)

    def add(target, where, q, right_ref):
        sl = spans[q]
        value = lax.dot_general(tail[where, sl], right_ref[:, sl], NT, preferred_element_type=jnp.float32)
        target[where, :] = value if q == 0 else target[where, :] + value

    for q in range(count):
        if q < shared:
            for copy in last[q]:
                copy.wait_recv()
            tail_relay[q].start()
            add(tail_gram, near_rows, q, own)
            add(acc, near_rows, q, upper)
        else:
            @pl.when(core == 1)
            def _():
                for copy in lead[q - shared]:
                    copy.wait_recv()
                for copy in lead_relay[q - shared]:
                    copy.start()
        if 0 < q <= shared:
            tail_relay[q - 1].wait_recv()
            add(tail_gram, relay_rows, q - 1, own)
        if q >= shared:
            @pl.when(core == 0)
            def _():
                for copy in lead_relay[q - shared]:
                    copy.wait_recv()

            add(tail_gram, pl.ds(0, 4 * late), q, own)
            add(acc, near_rows, q, upper)
    for s in (0, 1):
        g_ref[3, pl.ds(s * half + late_offset, late), :] = acc[pl.ds(s * late, late), :]
        keep_slot(tail_gram[pl.ds(s * late, late), :], s * half + late_offset, late)
    g_ref[3] = oriented(me, groups, g_ref[3], 3)

    sent = to_right + to_left + [to_sib] + relay[0] + relay[1] + far_relay + tail_relay
    for copy in sent + [copy for pair in fwd + last for copy in pair]:
        copy.wait_send()

    @pl.when(core == 1)
    def _():
        for copy in sum(lead + lead_relay, []):
            copy.wait_send()


def finish_kernel(y_ref, g_ref, tail_gram, tail, y_out, g_out, stage, y_sem, g_sem):
    cols = y_ref.shape[1]
    copies = [pltpu.make_async_copy(g_ref, g_out, g_sem)]
    copies[0].start()
    coef = tail_gram[...].astype(jnp.bfloat16).T
    width = cols // OUT_PARTS
    for part in range(OUT_PARTS):
        sl = pl.ds(part * width, width)
        stage[:, sl] = y_ref[:, sl] + jnp.dot(coef, tail[:, sl], preferred_element_type=jnp.float32)
        copy = pltpu.make_async_copy(stage.at[:, sl], y_out.at[:, sl], y_sem.at[part])
        copy.start()
        copies.append(copy)
    for copy in copies:
        copy.wait()


def solution(mesh):
    groups = mesh.shape["row"]

    def per_device(own_block):
        rows, cols = own_block.shape
        slots = groups // 2 + 1
        early, late = piece_rows(rows // 2)
        dma = pltpu.SemaphoreType.DMA
        whole = pl.BlockSpec(memory_space=pltpu.VMEM)
        raw = pl.BlockSpec(memory_space=pl.ANY)
        y_part, gram, tail_gram, tail, _ = pl.pallas_call(
            functools.partial(gather_kernel, groups),
            out_shape=(
                pltpu.VMEM((rows, cols), jnp.float32),
                pltpu.VMEM((slots, rows, rows), jnp.float32),
                pltpu.VMEM((4 * late, rows), jnp.float32),
                pltpu.VMEM((4 * late, cols), jnp.bfloat16),
                jax.ShapeDtypeStruct((5, rows, cols), jnp.bfloat16),
            ),
            in_specs=[raw],
            out_specs=(whole, whole, whole, whole, raw),
            scratch_shapes=[
                pltpu.VMEM((rows, cols), jnp.bfloat16),
                pltpu.VMEM((2 * rows, cols), jnp.bfloat16),
                pltpu.VMEM((4 * sum(early), cols), jnp.bfloat16),
                pltpu.VMEM((2 * rows, rows), jnp.float32),
                dma((5,)), dma((5,)),
                dma((2 * len(early),)), dma((2 * len(early),)),
                dma((4,)), dma((4,)),
                dma((len(early),)), dma((len(early),)),
                dma((2 * len(LAST_PARTS),)), dma((2 * len(LAST_PARTS),)),
                dma((len(LAST_PARTS),)), dma((len(LAST_PARTS),)),
                dma((6 * LEADS,)), dma((6 * LEADS,)),
                dma((12,)),
            ],
            compiler_params=pltpu.CompilerParams(
                collective_id=0, has_side_effects=True, vmem_limit_bytes=GATHER_VMEM),
        )(own_block)
        applied, gram = pl.pallas_call(
            finish_kernel,
            out_shape=(
                jax.ShapeDtypeStruct((rows, cols), jnp.float32),
                jax.ShapeDtypeStruct((slots, rows, rows), jnp.float32),
            ),
            in_specs=[whole, whole, whole, whole],
            out_specs=(raw, raw),
            scratch_shapes=[pltpu.VMEM((rows, cols), jnp.float32), dma((OUT_PARTS,)), dma],
            compiler_params=pltpu.CompilerParams(vmem_limit_bytes=FINISH_VMEM),
        )(y_part, gram, tail_gram, tail)
        return gram[None], applied

    return jax.shard_map(
        per_device, mesh=mesh, in_specs=(P(("mat", "row"), None),),
        out_specs=(P(("mat", "row"), None, None, None), P(("mat", "row"), None)), check_vma=False)
```

```python
import functools

import jax
import jax.numpy as jnp
from jax import lax
from jax.experimental import pallas as pl
from jax.experimental.pallas import tpu as pltpu
from jax.sharding import PartitionSpec as P

GRAM_STEP = 4096
APPLY_STEP = 2048
LAST_PARTS = (4, 4, 4, 4, 4, 4, 2, 4, 2)
LEADS = 2
OUT_PARTS = 16
GATHER_VMEM = 40 << 20
FINISH_VMEM = 18 << 20

NT = (((1,), (1,)), ((), ()))


def piece_rows(half):
    return (half // 2, half // 4), half // 4


def oriented(me, groups, value, slot):
    first_blk = lax.rem(me + slot % 2, groups)
    return jnp.where(first_blk + slot >= groups, value.T, value)


def gather_kernel(groups, a_ref, y_ref, g_ref, tail_gram, tail, hb, own, work, far, acc,
                  own_send, own_recv, fwd_send, fwd_recv, relay_send, relay_recv,
                  far_send, far_recv, last_send, last_recv, tail_send, tail_recv, lead_send, lead_recv, load_sem):
    rows, cols = a_ref.shape
    half = rows // 2
    early, late = piece_rows(half)
    me = lax.axis_index("row")
    core = lax.rem(me, 2)
    right = lax.rem(me + 2, groups)
    left = lax.rem(me + groups - 2, groups)
    sib = me + 1 - 2 * core

    def remote(src, dst, send, recv, to):
        return pltpu.make_async_remote_copy(
            src_ref=src, dst_ref=dst, send_sem=send, recv_sem=recv,
            device_id={"row": to}, device_id_type=pl.DeviceIdType.MESH)

    barrier = pltpu.get_barrier_semaphore()
    for peer in (left, right, sib):
        pl.semaphore_signal(barrier, inc=1, device_id={"row": peer}, device_id_type=pl.DeviceIdType.MESH)
    pl.semaphore_wait(barrier, 3)

    def half_rows(index):
        return pl.ds(index * half, half)

    to_right = [remote(a_ref.at[half_rows(s)], hb.at[1, half_rows(s)], own_send.at[s], own_recv.at[s], right) for s in (0, 1)]
    to_left = [remote(a_ref.at[half_rows(s)], hb.at[2, half_rows(s)], own_send.at[2 + s], own_recv.at[2 + s], left) for s in (0, 1)]
    to_sib = remote(a_ref, hb.at[0], own_send.at[4], own_recv.at[4], sib)
    to_right[0].start()
    to_left[1].start()
    to_right[1].start()
    to_left[0].start()
    to_sib.start()

    fwd, far_relay, batch, offset = [], [], [], 0
    for i, piece in enumerate(early):
        base = 4 * offset
        batch.append(far.at[pl.ds(base, 4 * piece)])
        fwd.append([remote(hb.at[1 + side, pl.ds(side * half + offset, piece)], far.at[pl.ds(base + side * piece, piece)],
                           fwd_send.at[2 * i + side], fwd_recv.at[2 * i + side], (right, left)[side]) for side in (0, 1)])
        far_relay.append(remote(far.at[pl.ds(base, 2 * piece)], far.at[pl.ds(base + 2 * piece, 2 * piece)],
                                far_send.at[i], far_recv.at[i], sib))
        offset += piece
    late_offset = offset
    count, unit = len(LAST_PARTS), cols // sum(LAST_PARTS)
    spans = [pl.ds(sum(LAST_PARTS[:q]) * unit, LAST_PARTS[q] * unit) for q in range(count)]
    last, tail_relay = [], []
    shared = count - LEADS
    for q, sl in enumerate(spans[:shared]):
        last.append([remote(hb.at[1 + side, pl.ds(side * half + late_offset, late), sl], tail.at[pl.ds(side * late, late), sl],
                            last_send.at[2 * q + side], last_recv.at[2 * q + side], (right, left)[side]) for side in (0, 1)])
        tail_relay.append(remote(tail.at[pl.ds(0, 2 * late), sl], tail.at[pl.ds(2 * late, 2 * late), sl],
                                 tail_send.at[q], tail_recv.at[q], sib))
    lead, lead_relay = [], []
    for q, sl in enumerate(spans[shared:]):
        lead.append([remote(hb.at[slot, pl.ds(side * half + late_offset, late), sl], tail.at[pl.ds((slot - 1) * late, late), sl],
                            lead_send.at[6 * q + slot - 1], lead_recv.at[6 * q + slot - 1], (right, left)[side])
                     for slot, side in ((1, 0), (2, 1), (3, 0), (4, 1))])
        lead_relay.append([remote(tail.at[pl.ds(2 * late * i, 2 * late), sl], tail.at[pl.ds(2 * late * (1 - i), 2 * late), sl],
                                  lead_send.at[6 * q + 4 + i], lead_recv.at[6 * q + 4 + i], sib) for i in (0, 1)])
    relay = [[remote(hb.at[1 + side, half_rows(s)], hb.at[3 + side, half_rows(s)],
                     relay_send.at[2 * side + s], relay_recv.at[2 * side + s], sib) for s in (0, 1)] for side in (0, 1)]

    def gram_t(left_ref, right_ref, count):
        acc[pl.ds(0, count), :] = jnp.zeros((count, rows), jnp.float32)

        def body(step, carry):
            sl = pl.ds(pl.multiple_of(step * GRAM_STEP, GRAM_STEP), GRAM_STEP)
            acc[pl.ds(0, count), :] += lax.dot_general(
                left_ref[:, sl], right_ref[:, sl], NT, preferred_element_type=jnp.float32)
            return carry

        lax.fori_loop(0, cols // GRAM_STEP, body, 0)

    def apply(b_ref, count, first=False):
        coef = acc[pl.ds(0, count), :].astype(jnp.bfloat16).T

        def body(step, carry):
            sl = pl.ds(pl.multiple_of(step * APPLY_STEP, APPLY_STEP), APPLY_STEP)
            term = jnp.dot(coef, b_ref[:, sl], preferred_element_type=jnp.float32)
            y_ref[:, sl] = term if first else y_ref[:, sl] + term
            return carry

        lax.fori_loop(0, cols // APPLY_STEP, body, 0)

    def load(src, dst, sem):
        copy = pltpu.make_async_copy(src, dst, sem)
        copy.start()
        return copy

    lower, upper = work.at[pl.ds(0, rows)], work.at[pl.ds(rows, rows)]
    load(a_ref, own, load_sem.at[0]).wait()
    gram_t(own, own, rows)
    g_ref[0] = acc[pl.ds(0, rows), :]
    apply(own, rows, first=True)

    to_sib.wait_recv()
    load(hb.at[0], lower, load_sem.at[1]).wait()
    gram_t(lower, own, rows)
    apply(lower, rows)

    for turn in (0, 1):
        arrivals = (to_right[turn], to_left[1 - turn])
        for copy in arrivals:
            copy.wait_recv()
        if turn == 0:
            for pair in fwd + last:
                for copy in pair:
                    copy.start()
        picks = (relay[0][turn], relay[1][1 - turn])
        for copy in picks:
            copy.start()
        halves = (half_rows(turn), half_rows(1 - turn))
        loads = [load(hb.at[1 + side, halves[side]], work.at[half_rows(side)], load_sem.at[2 + 4 * turn + side]) for side in (0, 1)]
        for side, copy in enumerate(picks):
            copy.wait_recv()
            loads.append(load(hb.at[3 + side, halves[side]], work.at[half_rows(2 + side)], load_sem.at[4 + 4 * turn + side]))
        if turn == 0:
            @pl.when(core == 1)
            def _():
                for copy in sum(lead, []):
                    copy.start()
        for copy in loads:
            copy.wait()
        gram_t(work, own, 2 * rows)
        g_ref[2, halves[1], :] = acc[half_rows(1), :]
        apply(work, 2 * rows)
    g_ref[2] = oriented(me, groups, g_ref[2], 2)

    pair_loads = [load(hb.at[2], lower, load_sem.at[10]), load(hb.at[4 * core], upper, load_sem.at[11])]

    def keep_slot(value, row, count):
        g_ref[4, pl.ds(row, count), :] = jnp.where(me >= groups // 2, 0.0, value)

    def next_gram(piece, offset):
        gram_t(far.at[pl.ds(4 * offset, 2 * piece)], upper, 2 * piece)
        for s in (0, 1):
            g_ref[3, pl.ds(s * half + offset, piece), :] = acc[pl.ds(s * piece, piece), :]

    offset = 0
    for i, piece in enumerate(early):
        for copy in fwd[i]:
            copy.wait_recv()
        far_relay[i].start()
        if i > 0:
            next_gram(piece, offset)
        far_relay[i].wait_recv()
        gram_t(batch[i], own, 4 * piece)
        for s in (0, 1):
            keep_slot(acc[pl.ds(s * piece, piece), :], s * half + offset, piece)
        apply(batch[i], 4 * piece)
        if i == 0:
            for copy in pair_loads:
                copy.wait()
            gram_t(lower, upper, rows)
            g_ref[1] = oriented(me, groups, acc[pl.ds(0, rows), :], 1)
            next_gram(piece, offset)
        offset += piece

    near_rows, relay_rows = pl.ds(0, 2 * late), pl.ds(2 * late, 2 * late)

    def add(target, where, q, right_ref):
        sl = spans[q]
        value = lax.dot_general(tail[where, sl], right_ref[:, sl], NT, preferred_element_type=jnp.float32)
        target[where, :] = value if q == 0 else target[where, :] + value

    for q in range(count):
        if q < shared:
            for copy in last[q]:
                copy.wait_recv()
            tail_relay[q].start()
            add(tail_gram, near_rows, q, own)
            add(acc, near_rows, q, upper)
        else:
            @pl.when(core == 1)
            def _():
                for i in (0, 1):
                    for copy in lead[q - shared][2 * i:2 * i + 2]:
                        copy.wait_recv()
                    lead_relay[q - shared][i].start()
        if 0 < q <= shared:
            tail_relay[q - 1].wait_recv()
            add(tail_gram, relay_rows, q - 1, own)
        if q >= shared:
            @pl.when(core == 0)
            def _():
                for copy in lead_relay[q - shared]:
                    copy.wait_recv()

            add(tail_gram, pl.ds(0, 4 * late), q, own)
            add(acc, near_rows, q, upper)
    for s in (0, 1):
        g_ref[3, pl.ds(s * half + late_offset, late), :] = acc[pl.ds(s * late, late), :]
        keep_slot(tail_gram[pl.ds(s * late, late), :], s * half + late_offset, late)
    g_ref[3] = oriented(me, groups, g_ref[3], 3)

    sent = to_right + to_left + [to_sib] + relay[0] + relay[1] + far_relay + tail_relay
    for copy in sent + [copy for pair in fwd + last for copy in pair]:
        copy.wait_send()

    @pl.when(core == 1)
    def _():
        for copy in sum(lead + lead_relay, []):
            copy.wait_send()


def finish_kernel(y_ref, g_ref, tail_gram, tail, y_out, g_out, stage, y_sem, g_sem):
    cols = y_ref.shape[1]
    copies = [pltpu.make_async_copy(g_ref, g_out, g_sem)]
    copies[0].start()
    coef = tail_gram[...].astype(jnp.bfloat16).T
    width = cols // OUT_PARTS
    for part in range(OUT_PARTS):
        sl = pl.ds(part * width, width)
        stage[:, sl] = y_ref[:, sl] + jnp.dot(coef, tail[:, sl], preferred_element_type=jnp.float32)
        copy = pltpu.make_async_copy(stage.at[:, sl], y_out.at[:, sl], y_sem.at[part])
        copy.start()
        copies.append(copy)
    for copy in copies:
        copy.wait()


def solution(mesh):
    groups = mesh.shape["row"]

    def per_device(own_block):
        rows, cols = own_block.shape
        slots = groups // 2 + 1
        early, late = piece_rows(rows // 2)
        dma = pltpu.SemaphoreType.DMA
        whole = pl.BlockSpec(memory_space=pltpu.VMEM)
        raw = pl.BlockSpec(memory_space=pl.ANY)
        y_part, gram, tail_gram, tail, _ = pl.pallas_call(
            functools.partial(gather_kernel, groups),
            out_shape=(
                pltpu.VMEM((rows, cols), jnp.float32),
                pltpu.VMEM((slots, rows, rows), jnp.float32),
                pltpu.VMEM((4 * late, rows), jnp.float32),
                pltpu.VMEM((4 * late, cols), jnp.bfloat16),
                jax.ShapeDtypeStruct((5, rows, cols), jnp.bfloat16),
            ),
            in_specs=[raw],
            out_specs=(whole, whole, whole, whole, raw),
            scratch_shapes=[
                pltpu.VMEM((rows, cols), jnp.bfloat16),
                pltpu.VMEM((2 * rows, cols), jnp.bfloat16),
                pltpu.VMEM((4 * sum(early), cols), jnp.bfloat16),
                pltpu.VMEM((2 * rows, rows), jnp.float32),
                dma((5,)), dma((5,)),
                dma((2 * len(early),)), dma((2 * len(early),)),
                dma((4,)), dma((4,)),
                dma((len(early),)), dma((len(early),)),
                dma((2 * len(LAST_PARTS),)), dma((2 * len(LAST_PARTS),)),
                dma((len(LAST_PARTS),)), dma((len(LAST_PARTS),)),
                dma((6 * LEADS,)), dma((6 * LEADS,)),
                dma((12,)),
            ],
            compiler_params=pltpu.CompilerParams(
                collective_id=0, has_side_effects=True, vmem_limit_bytes=GATHER_VMEM),
        )(own_block)
        applied, gram = pl.pallas_call(
            finish_kernel,
            out_shape=(
                jax.ShapeDtypeStruct((rows, cols), jnp.float32),
                jax.ShapeDtypeStruct((slots, rows, rows), jnp.float32),
            ),
            in_specs=[whole, whole, whole, whole],
            out_specs=(raw, raw),
            scratch_shapes=[pltpu.VMEM((rows, cols), jnp.float32), dma((OUT_PARTS,)), dma],
            compiler_params=pltpu.CompilerParams(vmem_limit_bytes=FINISH_VMEM),
        )(y_part, gram, tail_gram, tail)
        return gram[None], applied

    return jax.shard_map(
        per_device, mesh=mesh, in_specs=(P(("mat", "row"), None),),
        out_specs=(P(("mat", "row"), None, None, None), P(("mat", "row"), None)), check_vma=False)
```
